512 devices in a mesh: sub: 64 (over y, x, core), crs: 8 (over z).
Axes of the slice: x: 4, y: 8, z: 8, core: 2. Of those that a mesh axis runs over, the one named last changes fastest.
Arguments:
- multipliers: float32 [16, 2048, 512], P(None, ('sub', 'crs')), may hold values from -6 to 6
- own_modes: float32 [6, 2048, 512], P(None, ('sub', 'crs')), may hold values from -0.75 to 0.75
- neighbour_modes: float32 [6, 2048, 512], P(None, ('sub', 'crs')), may hold values from -0.75 to 0.75
- face_index: int32 [2048, 512], P(('sub', 'crs')), may hold values from 0 to 5, as said below
- neighbour_list: int32 [2048, 6], replicated, may hold values from 0 to 2047, as said below
- coarse_factor: float32 [12288, 12288], P('sub', 'crs'), may hold values from -0.0546875 to 0.0546875
Outputs:
- projected: float32 [16, 2048, 512], P(None, ('sub', 'crs'))
The draws below stay inside these ranges and needn't reach their ends.
Inputs may be any that keep to these rules, and one draw needn't show every extreme that they name: `face_index`: the multipliers of each subdomain lie in 6 contiguous nonempty blocks, face 0 first and face 5 last. `neighbour_list`: subdomain s = (32 x + y) * 32 + z sits at (x, y, z) of a periodic grid of 2 x 32 x 32 subdomains; the 6 faces of each subdomain name its grid neighbours x plus 1, x minus 1, y plus or minus 1, z plus or minus 1 (periodic; along the first dimension both name the same subdomain), in an order that differs from subdomain to subdomain.
All inputs are finite; a program needn't handle non-finite values.
Results may differ from the reference program's by a relative error of at most 0.0001.
Values sent between devices are 32-bit elements; how exact they have to be, the bound alone decides.
A program may use at most 64 MiB of HBM per device.

```python
import jax
import jax.numpy as jnp
from jax import lax

MODES = 6
NFACE = 6
IW = 512
NRHS = 16
NSUB = 2048
NC = 12288
GY = 32
GX = 2
GZ = 32


def draw_face_index(key, part):
    block = IW // NFACE
    spread = block // 4
    jitter = jax.random.randint(key, (NSUB, NFACE - 1), -spread, spread + 1).astype(jnp.int32)
    starts = (lax.broadcasted_iota(jnp.int32, (NSUB, NFACE - 1), 1) + 1) * block + jitter
    places = lax.broadcasted_iota(jnp.int32, (NSUB, IW), 1)
    passed = (places[:, :, None] >= starts[:, None, :]).astype(jnp.int32)
    return jnp.sum(passed, axis=2).astype(jnp.int32)


def draw_neighbour_list(key, part):
    scores = jax.random.randint(jax.random.fold_in(key, 17), (NSUB, NFACE), 0, 1 << 20).astype(jnp.int32)
    scores = scores * 8 + lax.broadcasted_iota(jnp.int32, (NSUB, NFACE), 1)
    order = jnp.argsort(scores, axis=1, stable=True).astype(jnp.int32)
    cells = lax.iota(jnp.int32, NSUB)
    first = cells // (GY * GZ)
    second = cells // GZ % GY
    third = cells % GZ

    def place(a, b, c):
        return ((a * GY + b) * GZ + c).astype(jnp.int32)
    table = jnp.stack([place((first + 1) % GX, second, third), place((first + GX - 1) % GX, second, third), place(first, (second + 1) % GY, third), place(first, (second + GY - 1) % GY, third), place(first, second, (third + 1) % GZ), place(first, second, (third + GZ - 1) % GZ)], axis=1)
    return jnp.take_along_axis(table, order, axis=1).astype(jnp.int32)


def levels(stream_key, dims, cuts, low, top_value):
    gain = 1.0
    for dim, parts in cuts:
        draws = jax.random.uniform(jax.random.fold_in(jax.random.fold_in(stream_key, 6), dim), (parts,), jnp.float32, low / len(cuts), top_value / len(cuts))
        gain = gain * jnp.repeat(jnp.exp(draws), dims[dim] // parts).reshape((-1,) + (1,) * (len(dims) - 1 - dim))
    return gain


def normal_values(key, shape, scale, most, shards=(), kind=jnp.bfloat16):
    array = jax.random.normal(key, shape, jnp.float32) * scale
    if len(shards) > 0:
        array = levels(key, shape, shards, -0.22, 0.18) * array
    return jnp.clip(array, min=-most, max=most).astype(kind)


def setup_inputs(seed: int = 0) -> dict:
    seeds = jax.random.split(jax.random.key(seed), 7)
    return {
        "multipliers": normal_values(seeds[0], (NRHS, NSUB, IW), 1.0, 6.0, ((1, 512),), jnp.float32),
        "own_modes": normal_values(seeds[1], (MODES, NSUB, IW), (IW // 8) ** -0.5, 0.75, ((1, 512),), jnp.float32),
        "neighbour_modes": normal_values(seeds[2], (MODES, NSUB, IW), (IW // 8) ** -0.5, 0.75, ((1, 512),), jnp.float32),
        "face_index": draw_face_index(jax.random.fold_in(seeds[6], 71), 0),
        "neighbour_list": draw_neighbour_list(jax.random.fold_in(seeds[6], 71), 0),
        "coarse_factor": normal_values(seeds[5], (NC, NC), NC ** -0.5, 0.0546875, ((0, 64), (1, 8)), jnp.float32),
    }


HIGHEST = lax.Precision.HIGHEST


def reference(multipliers, own_modes, neighbour_modes, face_index, neighbour_list, coarse_factor):
    masked_modes = []
    for which_face in range(NFACE):
        masked_modes.append(neighbour_modes * (face_index == which_face).astype(jnp.float32)[None])
    coarse = jnp.einsum('ksm,rsm->krs', own_modes, multipliers, precision=HIGHEST)
    face_parts = []
    for which_face in range(NFACE):
        face_parts.append(jnp.einsum('ksm,rsm->krs', masked_modes[which_face], multipliers, precision=HIGHEST))
    face_terms = jnp.stack(face_parts, axis=3)
    flattened = face_terms.reshape(MODES, NRHS, NSUB * NFACE).transpose(2, 0, 1)
    targets = neighbour_list.reshape(NSUB * NFACE)
    incoming = jax.ops.segment_sum(flattened, targets, num_segments=NSUB)
    coarse = coarse + incoming.transpose(1, 2, 0)
    right_side = coarse.transpose(2, 0, 1).reshape(NSUB * MODES, NRHS)
    halfway = jnp.einsum('cp,cr->pr', coarse_factor, right_side, precision=HIGHEST)
    amplitudes = jnp.dot(coarse_factor, halfway, precision=HIGHEST, preferred_element_type=jnp.float32)
    amplitudes = amplitudes.reshape(NSUB, MODES, NRHS).transpose(1, 2, 0)
    applied = jnp.einsum('ksm,krs->rsm', own_modes, amplitudes, precision=HIGHEST)
    for which_face in range(NFACE):
        across = amplitudes[:, :, neighbour_list[:, which_face]]
        applied = applied + jnp.einsum('ksm,krs->rsm', masked_modes[which_face], across, precision=HIGHEST)
    return multipliers - applied
```

```python
import functools

import jax
import jax.numpy as jnp
from jax import lax
from jax.experimental import pallas as pl
from jax.experimental.pallas import tpu as pltpu
from jax.sharding import PartitionSpec as P

MODES = 6
NFACE = 6
PAD = 8
BLOCK = 32
F32 = jnp.float32
BF16 = jnp.bfloat16


def split(value):
    high = value.astype(BF16)
    return high, (value - high.astype(F32)).astype(BF16)


def dot3(value, high, low, transposed=False):
    rows = value.shape[0]
    first, second = split(value)
    dims = (((1,), (1 if transposed else 0,)), ((), ()))
    both = jnp.concatenate([first, second], axis=0)
    top = lax.dot_general(both, high, dims, preferred_element_type=F32)
    rest = lax.dot_general(first, low, dims, preferred_element_type=F32)
    return top[:rows] + top[rows:] + rest


def swap_blocks(parts):
    block = lax.broadcasted_iota(jnp.int32, parts[0].shape, 1) // BLOCK
    turned = [
        [part if by == 0 else pltpu.roll(part, BLOCK * by, 1) for by in range(4)] for part in parts
    ]
    out = []
    for q in range(4):
        value = turned[3][(3 - q) % 4]
        for d in (2, 1, 0):
            value = jnp.where(block == d, turned[d][(d - q) % 4], value)
        out.append(value)
    return out


def row_blocks(value):
    return [value[4 * q : 4 * q + 4] for q in range(4)]


def kernel(
    mult_h, own_h, near_h, face_h, list_h, coarse_h, out_h,
    mult, own, near, face, nlist, coarse, result,
    m_high, m_low, c_high, c_low,
    halo_out, halo_in, group, part_out, part_in, column, panel,
    amp_out, amp_in, side_out, side_in,
    load_sem, store_sem, send_sem, recv_sem,
):
    sub, crs = lax.axis_index("sub"), lax.axis_index("crs")
    y, xc = sub // 8, lax.rem(sub, 8)
    half, second = sub // 32, lax.rem(sub, 32)
    x_sub = lax.rem(sub + 32, 64)
    up_sub = half * 32 + lax.rem(second + 1, 32)
    down_sub = half * 32 + lax.rem(second + 31, 32)

    barrier = pltpu.get_barrier_semaphore()
    greeted = [(up_sub, crs), (down_sub, crs)]
    for k in range(1, 8):
        greeted.append((lax.rem(sub + 8 * k, 64), crs))
        greeted.append((sub, lax.rem(crs + k, 8)))
        greeted.append((y * 8 + lax.rem(xc + k, 8), crs))
    for peer in greeted:
        pl.semaphore_signal(barrier, inc=1, device_id=peer, device_id_type=pl.DeviceIdType.MESH)

    list_row = pl.multiple_of(sub * 32 + crs // 2 * 8, 8)
    loads = [
        pltpu.make_async_copy(src, dst, load_sem.at[i])
        for i, (src, dst) in enumerate(
            [
                (list_h.at[pl.ds(list_row, 8)], nlist),
                (face_h, face),
                (near_h, near),
                (own_h, own),
                (mult_h, mult),
                (coarse_h, coarse),
            ]
        )
    ]
    for load in loads:
        load.start()

    def send(src, dst, stage, peer):
        copy = pltpu.make_async_remote_copy(
            src_ref=src,
            dst_ref=dst,
            send_sem=send_sem.at[stage],
            recv_sem=recv_sem.at[stage],
            device_id=peer,
            device_id_type=pl.DeviceIdType.MESH,
        )
        copy.start()

    def landed(ref, stage):
        pltpu.make_async_copy(ref, ref, recv_sem.at[stage]).wait()

    def left(ref, stage):
        pltpu.make_async_copy(ref, ref, send_sem.at[stage]).wait()

    for i in range(4):
        loads[i].wait()
    rows = jnp.where(lax.rem(crs, 2) == 0, nlist[0:4, :], nlist[4:8, :])
    faces = face[...]
    across = jnp.zeros(faces.shape, jnp.int32)
    for which in range(NFACE):
        across = jnp.where(faces == which, rows[:, which : which + 1], across)
    third = crs * 4 + lax.broadcasted_iota(jnp.int32, faces.shape, 0)

    def place(group_index, c):
        return group_index * 32 + c

    targets = [
        place(x_sub, third),
        place(up_sub, third),
        place(down_sub, third),
        place(sub, lax.rem(third + 1, 32)),
        place(sub, lax.rem(third + 31, 32)),
    ]
    masks = [(across == target).astype(F32) for target in targets]
    blank = jnp.zeros((PAD, faces.shape[1]), F32)
    spare = jnp.zeros((PAD - MODES, faces.shape[1]), F32)
    loads[4].wait()
    sums = jnp.zeros((16, 160), F32)
    for j in range(4):
        near_j = jnp.concatenate([near[:, j, :], spare], axis=0)
        own_j = jnp.concatenate([own[:, j, :], spare], axis=0)
        seen = [near_j * mask[j : j + 1, :] for mask in masks]
        blocks = [blank] * 20
        blocks[j] = own_j
        for d in range(3):
            blocks[4 * (d + 1) + j] = seen[d]
        blocks[j + 1 if j < 3 else 16] = seen[3]
        blocks[j - 1 if j > 0 else 19] = seen[4]
        high, low = split(jnp.concatenate(blocks, axis=0))
        m_high[j] = high
        m_low[j] = low
        sums += dot3(mult[:, j, :], high, low, transposed=True)

    packed = swap_blocks(row_blocks(sums[:, :128]))
    edge = jnp.concatenate([sums[:, 128:], jnp.zeros((16, 96), F32)], axis=1)
    block4 = lax.broadcasted_iota(jnp.int32, (4, 128), 1)
    edges = row_blocks(edge)
    packed_edge = edges[0]
    for q in range(1, 4):
        packed_edge = jnp.where(block4 // BLOCK == q, pltpu.roll(edges[q], BLOCK * q, 1), packed_edge)
    for d in range(3):
        halo_out[d] = packed[d + 1]
    halo_out[3] = packed_edge

    pl.semaphore_wait(barrier, len(greeted))

    send(halo_out.at[0], halo_in.at[0], 0, (x_sub, crs))
    send(halo_out.at[1], halo_in.at[1], 0, (up_sub, crs))
    send(halo_out.at[2], halo_in.at[2], 0, (down_sub, crs))
    send(halo_out.at[3], halo_in.at[3], 0, (sub, lax.rem(crs + 1, 8)))
    send(halo_out.at[3], halo_in.at[4], 0, (sub, lax.rem(crs + 7, 8)))

    loads[5].wait()
    space = jnp.zeros((PAD - MODES, coarse.shape[1]), F32)
    for c in range(8):
        pieces = []
        for j in range(4):
            at = 24 * c + 6 * j
            pieces += [coarse[at : at + MODES, :], space]
        high, low = split(jnp.concatenate(pieces, axis=0))
        c_high[BLOCK * c : BLOCK * c + BLOCK, :] = high
        c_low[BLOCK * c : BLOCK * c + BLOCK, :] = low

    landed(halo_in, 0)
    lane = lax.rem(block4, BLOCK)
    chunk = packed[0] + halo_in[0] + halo_in[1] + halo_in[2]
    chunk += jnp.where(lane < PAD, halo_in[3], 0.0) + jnp.where(lane >= 24, halo_in[4], 0.0)
    group[crs] = chunk
    for k in range(1, 8):
        send(group.at[crs], group.at[crs], 1, (sub, lax.rem(crs + k, 8)))
    landed(group.at[pl.ds(0, 7)], 1)

    halves = []
    for h in range(2):
        halves.append(jnp.concatenate(swap_blocks([group[4 * h + d] for d in range(4)]), axis=0))
    rhs = jnp.concatenate(halves, axis=1)
    partial = dot3(rhs, c_high[...], c_low[...])
    for i in range(8):
        h, g = i // 4, i % 4
        part_out[i] = partial[8 * h : 8 * h + 8, 384 * g : 384 * g + 384]
    for k in range(1, 8):
        peer = lax.rem(xc + k, 8)
        send(part_out.at[peer], part_in.at[xc], 2, (y * 8 + peer, crs))
    part_in[xc] = part_out[xc]
    landed(part_in.at[pl.ds(0, 7)], 2)

    def total(ref):
        value = ref[0]
        for i in range(1, 8):
            value = value + ref[i]
        return value

    column[y] = total(part_in)
    for k in range(1, 8):
        send(column.at[y], column.at[y], 3, (lax.rem(y + k, 8) * 8 + xc, crs))
    landed(column.at[pl.ds(0, 7)], 3)
    panel[xc] = total(column)
    for k in range(1, 8):
        send(panel.at[xc], panel.at[xc], 4, (y * 8 + lax.rem(xc + k, 8), crs))
    landed(panel.at[pl.ds(0, 7)], 4)

    whole = jnp.concatenate(
        [jnp.concatenate([panel[4 * h + g] for g in range(4)], axis=1) for h in range(2)], axis=0
    )
    amps = dot3(whole, c_high[...], c_low[...], transposed=True)
    ready = []
    for h in range(2):
        ready += swap_blocks(row_blocks(amps[:, 128 * h : 128 * h + 128]))
    for c in range(8):
        side_out[c] = ready[c]
        rim = jnp.where(lane < PAD, ready[(c + 1) % 8], ready[(c + 7) % 8])
        amp_out[c] = jnp.concatenate([ready[c], rim], axis=0)
    for k in range(8):
        send(side_out.at[k], side_in.at[0, crs], 6, (x_sub, k))
        send(side_out.at[k], side_in.at[2, crs], 6, (up_sub, k))
        send(side_out.at[k], side_in.at[1, crs], 6, (down_sub, k))
    for k in range(1, 8):
        peer = lax.rem(crs + k, 8)
        send(amp_out.at[peer], amp_in.at[crs], 5, (sub, peer))
    amp_in[crs] = amp_out[crs]
    landed(amp_in.at[pl.ds(0, 7)], 5)
    landed(side_in, 6)

    mine = total(amp_in)
    sides = [total(side_in.at[d]) for d in range(3)]
    main = jnp.concatenate(swap_blocks([mine[0:4]] + sides), axis=0)
    rims = [mine[4:8]] + [pltpu.roll(mine[4:8], 128 - BLOCK * q, 1) for q in range(1, 4)]
    rim = jnp.concatenate(rims, axis=0)[:, :BLOCK]
    lhs = jnp.concatenate([main, rim], axis=1)
    for j in range(4):
        applied = dot3(lhs, m_high[j], m_low[j])
        result[:, j, :] = mult[:, j, :] - applied
    store = pltpu.make_async_copy(result, out_h, store_sem)
    store.start()
    left(halo_in, 0)
    left(group.at[pl.ds(0, 7)], 1)
    left(part_in.at[pl.ds(0, 7)], 2)
    left(column.at[pl.ds(0, 7)], 3)
    left(panel.at[pl.ds(0, 7)], 4)
    left(amp_in.at[pl.ds(0, 7)], 5)
    left(side_in, 6)
    store.wait()


def body(multipliers, own_modes, neighbour_modes, face_index, neighbour_list, coarse_factor):
    anywhere = pl.BlockSpec(memory_space=pl.ANY)
    rows, columns = coarse_factor.shape
    width = face_index.shape[1]
    return pl.pallas_call(
        kernel,
        out_shape=jax.ShapeDtypeStruct(multipliers.shape, F32),
        in_specs=[anywhere] * 6,
        out_specs=anywhere,
        scratch_shapes=[
            pltpu.VMEM(multipliers.shape, F32),
            pltpu.VMEM(own_modes.shape, F32),
            pltpu.VMEM(own_modes.shape, F32),
            pltpu.VMEM(face_index.shape, jnp.int32),
            pltpu.VMEM((8, NFACE), jnp.int32),
            pltpu.VMEM((rows, columns), F32),
            pltpu.VMEM(multipliers.shape, F32),
            pltpu.VMEM((4, 160, width), BF16),
            pltpu.VMEM((4, 160, width), BF16),
            pltpu.VMEM((256, columns), BF16),
            pltpu.VMEM((256, columns), BF16),
            pltpu.VMEM((4, 4, 128), F32),
            pltpu.VMEM((5, 4, 128), F32),
            pltpu.VMEM((8, 4, 128), F32),
            pltpu.VMEM((8, 8, 384), F32),
            pltpu.VMEM((8, 8, 384), F32),
            pltpu.VMEM((8, 8, 384), F32),
            pltpu.VMEM((8, 8, 384), F32),
            pltpu.VMEM((8, 8, 128), F32),
            pltpu.VMEM((8, 8, 128), F32),
            pltpu.VMEM((8, 4, 128), F32),
            pltpu.VMEM((3, 8, 4, 128), F32),
            pltpu.SemaphoreType.DMA((6,)),
            pltpu.SemaphoreType.DMA,
            pltpu.SemaphoreType.DMA((7,)),
            pltpu.SemaphoreType.DMA((7,)),
        ],
        compiler_params=pltpu.CompilerParams(collective_id=0, has_side_effects=True),
    )(multipliers, own_modes, neighbour_modes, face_index, neighbour_list, coarse_factor)


def solution(mesh):
    placed = (
        P(None, ("sub", "crs"), None),
        P(None, ("sub", "crs"), None),
        P(None, ("sub", "crs"), None),
        P(("sub", "crs"), None),
        P(),
        P("sub", "crs"),
    )
    return jax.shard_map(
        body, mesh=mesh, in_specs=placed, out_specs=P(None, ("sub", "crs"), None), check_vma=False
    )
```

```python
import functools

import jax
import jax.numpy as jnp
from jax import lax
from jax.experimental import pallas as pl
from jax.experimental.pallas import tpu as pltpu
from jax.sharding import PartitionSpec as P

MODES = 6
NFACE = 6
BLOCK = 32
F32 = jnp.float32
BF16 = jnp.bfloat16


def split(value):
    high = value.astype(BF16)
    return high, (value - high.astype(F32)).astype(BF16)


def dot3(value, high, low, transposed=False):
    rows = value.shape[0]
    first, second = split(value)
    dims = (((1,), (1 if transposed else 0,)), ((), ()))
    both = jnp.concatenate([first, second], axis=0)
    top = lax.dot_general(both, high, dims, preferred_element_type=F32)
    rest = lax.dot_general(first, low, dims, preferred_element_type=F32)
    return top[:rows] + top[rows:] + rest


def swap_blocks(parts):
    block = lax.broadcasted_iota(jnp.int32, parts[0].shape, 1) // BLOCK
    turned = [
        [part if by == 0 else pltpu.roll(part, BLOCK * by, 1) for by in range(4)] for part in parts
    ]
    out = []
    for q in range(4):
        value = turned[3][(3 - q) % 4]
        for d in (2, 1, 0):
            value = jnp.where(block == d, turned[d][(d - q) % 4], value)
        out.append(value)
    return out


def row_blocks(value):
    return [value[4 * q : 4 * q + 4] for q in range(4)]


def all_sends(n):
    return sorted(range(1, n), key=lambda k: -min(k, n - k))


def kernel(
    mult_h, own_h, near_h, face_h, list_h, coarse_h, result,
    local, face, nlist, coarse,
    m_high, m_low, c_high, c_low, t_high, t_low,
    halo_out, halo_in, group, part_out, part_in, column, panel,
    amp_out, amp_in, side_out, side_in, early,
    load_sem, send_sem, recv_sem, ready_sem,
):
    sub, crs = lax.axis_index("sub"), lax.axis_index("crs")
    y, xc = sub // 8, lax.rem(sub, 8)
    half, second = sub // 32, lax.rem(sub, 32)
    x_sub = lax.rem(sub + 32, 64)
    up_sub = half * 32 + lax.rem(second + 1, 32)
    down_sub = half * 32 + lax.rem(second + 31, 32)
    ring = all_sends(8)

    barrier = pltpu.get_barrier_semaphore()

    def greet(peer):
        pl.semaphore_signal(barrier, inc=1, device_id=peer, device_id_type=pl.DeviceIdType.MESH)

    along_z = [(k, lax.rem(crs + k, 8)) for k in (4, 3, 5, 2, 6)]
    along_y = [(k, lax.rem(y + k, 8)) for k in (3, 5, 2, 6, 1, 7)]
    chip, core = xc // 2, lax.rem(xc, 2)
    along_x = [
        (k, lax.rem(chip + k, 4) * 2 + (core if same else 1 - core))
        for k, same in ((2, 1), (2, 0), (1, 1), (1, 0), (3, 1), (3, 0), (0, 0))
    ]
    classes = [
        (along_z, crs, ready_sem.at[0], lambda at: (sub, at)),
        (along_y, y, ready_sem.at[1], lambda at: (at * 8 + xc, crs)),
        (along_x, xc, ready_sem.at[2], lambda at: (y * 8 + at, crs)),
    ]
    greet((x_sub, crs))
    greet((up_sub, crs))
    greet((down_sub, crs))
    greet((sub, lax.rem(crs + 1, 8)))
    greet((sub, lax.rem(crs + 7, 8)))

    list_at = pl.multiple_of(sub // 4 * 128, 128)
    loads = [
        (list_h, nlist, 0),
        (face_h, face, 1),
        (near_h, local.at[pl.ds(MODES, MODES)], 2),
        (own_h, local.at[pl.ds(0, MODES)], 2),
        (mult_h, local.at[pl.ds(2 * MODES, 16)], 2),
    ]
    for src, dst, i in loads:
        pltpu.make_async_copy(src, dst, load_sem.at[i]).start()
    expected = jnp.int32(5)
    for peers, mine, _, where in classes:
        for _, at in peers:
            pl.when(at > mine)(functools.partial(lambda where, at: greet(where(at)), where, at))
            expected += jnp.where(at < mine, 1, 0)
    pltpu.make_async_copy(coarse_h, coarse, load_sem.at[3]).start()

    def tell(ready, where, at):
        pl.semaphore_signal(
            ready, inc=1, device_id=where(at), device_id_type=pl.DeviceIdType.MESH
        )

    def heard(which):
        peers, mine, ready, _ = classes[which]
        higher = jnp.int32(0)
        for _, at in peers:
            higher += jnp.where(at > mine, 1, 0)
        pl.when(higher > 0)(lambda: pl.semaphore_wait(ready, higher))

    def send(src, dst, stage, peer):
        copy = pltpu.make_async_remote_copy(
            src_ref=src,
            dst_ref=dst,
            send_sem=send_sem,
            recv_sem=recv_sem.at[stage],
            device_id=peer,
            device_id_type=pl.DeviceIdType.MESH,
        )
        copy.start()

    def loaded(ref, which):
        pltpu.make_async_copy(ref, ref, load_sem.at[which]).wait()

    def landed(ref, stage):
        pltpu.make_async_copy(ref, ref, recv_sem.at[stage]).wait()

    loaded(nlist, 0)
    loaded(face, 1)
    shift = lax.rem(sub, 4) * 32 + crs * 4
    lists = pltpu.roll(nlist[:, pl.ds(list_at, 128)], lax.rem(128 - shift, 128), 1).astype(F32)
    faces = face[...]
    width = faces.shape[1]
    which = lax.broadcasted_iota(jnp.int32, (NFACE, width), 0)
    across = []
    for j in range(4):
        named = jnp.where(faces[j : j + 1, :] == which, lists[:, j : j + 1], 0.0)
        across.append(jnp.sum(named, axis=0, keepdims=True))
    across = jnp.concatenate(across, axis=0).astype(jnp.int32)
    third = crs * 4 + lax.broadcasted_iota(jnp.int32, faces.shape, 0)
    targets = [
        x_sub * 32 + third,
        up_sub * 32 + third,
        down_sub * 32 + third,
        sub * 32 + lax.rem(third + 1, 32),
        sub * 32 + lax.rem(third + 31, 32),
    ]
    loaded(local, 2)
    blank = jnp.zeros((8, width), F32)
    stack = [local[k] for k in range(MODES)] + [blank]
    for target in targets:
        hit = across == target
        stack += [jnp.where(hit, local[MODES + k], 0.0) for k in range(MODES)] + [blank]
    high, low = split(jnp.concatenate(stack, axis=0))
    m_high[...] = high
    m_low[...] = low
    values = jnp.concatenate([local[2 * MODES + r] for r in range(16)], axis=0)
    every = dot3(values, high, low, transposed=True)
    mine_rows = lax.broadcasted_iota(jnp.int32, every.shape, 0) % 4
    mine_lanes = lax.broadcasted_iota(jnp.int32, every.shape, 1) % 4
    same = mine_rows == mine_lanes
    sums = jnp.sum(jnp.where(same, every, 0.0).reshape(16, 4, 192), axis=1)

    packed = swap_blocks(row_blocks(sums[:, :128]))
    tail = jnp.concatenate([sums[:, 128:], jnp.zeros((16, 64), F32)], axis=1)
    above, below = swap_blocks(row_blocks(tail))[:2]
    place = lax.rem(lax.broadcasted_iota(jnp.int32, (4, 128), 1), 4)
    for d in range(3):
        halo_out[d] = packed[d + 1]
    crossing = jnp.where(place == 3, pltpu.roll(below, 3, 1), 0.0)
    halo_out[3] = jnp.where(place == 0, pltpu.roll(above, 125, 1), crossing)

    pl.semaphore_wait(barrier, expected)
    send(halo_out.at[0], halo_in.at[0], 0, (x_sub, crs))
    send(halo_out.at[1], halo_in.at[1], 0, (up_sub, crs))
    send(halo_out.at[2], halo_in.at[2], 0, (down_sub, crs))
    send(halo_out.at[3], halo_in.at[3], 0, (sub, lax.rem(crs + 1, 8)))
    send(halo_out.at[3], halo_in.at[4], 0, (sub, lax.rem(crs + 7, 8)))
    for peers, mine, ready, where in classes:
        for _, at in peers:
            pl.when(at < mine)(functools.partial(tell, ready, where, at))

    chunk = packed[0] + jnp.where(place > 0, pltpu.roll(above, 1, 1), 0.0)
    chunk += jnp.where(place < 3, pltpu.roll(below, 127, 1), 0.0)

    space = jnp.zeros((8, 128), F32)
    loaded(coarse, 3)
    for g in range(12):
        for c in range(8):
            lanes = slice(128 * g, 128 * g + 128)
            at = [24 * c + 6 * j + k for k in range(MODES) for j in range(4)]
            rows = [coarse[i : i + 1, lanes] for i in at]
            high, low = split(jnp.concatenate(rows + [space], axis=0))
            c_high[BLOCK * c : BLOCK * c + BLOCK, 128 * g : 128 * g + 128] = high
            c_low[BLOCK * c : BLOCK * c + BLOCK, 128 * g : 128 * g + 128] = low

    landed(halo_in, 0)
    chunk += halo_in[0] + halo_in[1] + halo_in[2]
    chunk += jnp.where(place == 0, halo_in[3], 0.0) + jnp.where(place == 3, halo_in[4], 0.0)
    group[crs] = chunk
    for k in (1, 7):
        send(group.at[crs], group.at[crs], 1, (sub, lax.rem(crs + k, 8)))
    heard(0)
    for k, at in along_z:
        send(group.at[crs], group.at[crs], 1 if k in (2, 6) else 6, (sub, at))
    for h in range(2):
        t_high[:, 128 * h : 128 * h + 128] = c_high[128 * h : 128 * h + 128, :].T
        t_low[:, 128 * h : 128 * h + 128] = c_low[128 * h : 128 * h + 128, :].T

    def gathered(wave):
        blocks = [lax.rem(crs + k, 8) for k in wave]
        chunks = [group[c] for c in blocks]
        chunks += [jnp.zeros((4, 128), F32)] * (-len(wave) % 4)
        lhs = [
            jnp.concatenate(swap_blocks(chunks[i : i + 4]), axis=0)
            for i in range(0, len(chunks), 4)
        ]
        lhs = jnp.concatenate(lhs, axis=1)[:, : BLOCK * len(wave)]
        return lhs, [pl.ds(pl.multiple_of(BLOCK * c, BLOCK), BLOCK) for c in blocks]

    def product(lhs, at, lanes):
        high = jnp.concatenate([c_high[rows, lanes] for rows in at], axis=0)
        low = jnp.concatenate([c_low[rows, lanes] for rows in at], axis=0)
        return dot3(lhs, high, low)

    heard(2)
    landed(group.at[pl.ds(0, 4)], 1)
    early[...] = product(*gathered((0, 1, 7, 2, 6)), slice(None))
    landed(group.at[pl.ds(0, 3)], 6)
    late = gathered((3, 5, 4))
    side = lax.rem(chip, 2)
    for step, which in enumerate((side, 1 - side)):
        lanes = pl.ds(pl.multiple_of(which * 768, 768), 768)
        partial = early[:, lanes] + product(*late, lanes)
        for h in range(2):
            for g in range(2):
                piece = partial[8 * h : 8 * h + 8, 384 * g : 384 * g + 384]
                part_out[4 * h + 2 * which + g] = piece
        for k, peer in along_x:
            if (k in (0, 2)) == (step == 0):
                send(part_out.at[peer], part_in.at[xc], 2, (y * 8 + peer, crs))
    part_in[xc] = part_out[xc]
    heard(1)
    landed(part_in.at[pl.ds(0, 7)], 2)

    def total(ref):
        value = ref[0]
        for i in range(1, 8):
            value = value + ref[i]
        return value

    column[y] = total(part_in)
    send(column.at[y], column.at[y], 3, (x_sub, crs))
    for _, at in along_y:
        send(column.at[y], column.at[y], 3, (at * 8 + xc, crs))
    landed(column.at[pl.ds(0, 7)], 3)
    panel[xc] = total(column)
    for _, peer in along_x:
        send(panel.at[xc], panel.at[xc], 4, (y * 8 + peer, crs))
    landed(panel.at[pl.ds(0, 7)], 4)

    whole = jnp.concatenate(
        [jnp.concatenate([panel[4 * h + g] for g in range(4)], axis=1) for h in range(2)], axis=0
    )
    ready = []
    for h in range(2):
        lanes = slice(128 * h, 128 * h + 128)
        ready += swap_blocks(row_blocks(dot3(whole, t_high[:, lanes], t_low[:, lanes])))
        for c in range(4 * h, 4 * h + 4):
            side_out[c] = ready[c]
        for c in range(4 * h, 4 * h + 4):
            send(side_out.at[c], side_in.at[0, crs], 7, (x_sub, c))
        for c in range(4 * h, 4 * h + 4):
            send(side_out.at[c], side_in.at[2, crs], 7, (up_sub, c))
            send(side_out.at[c], side_in.at[1, crs], 7, (down_sub, c))
    for c in range(8):
        rim = jnp.where(place == 0, ready[(c + 1) % 8], ready[(c + 7) % 8])
        amp_out[c] = jnp.concatenate([ready[c], rim], axis=0)
    for k in ring:
        peer = lax.rem(crs + k, 8)
        send(amp_out.at[peer], amp_in.at[crs], 5, (sub, peer))
    amp_in[crs] = amp_out[crs]
    def applied(parts, rows):
        parts = parts + [jnp.zeros((4, 128), F32)]
        lhs = jnp.concatenate(swap_blocks(parts), axis=0)[:, :96]
        lhs = jnp.broadcast_to(lhs[:, None, :], (16, 4, 96)).reshape(64, 96)
        high = jnp.concatenate([m_high[at, :] for at in rows], axis=0)
        low = jnp.concatenate([m_low[at, :] for at in rows], axis=0)
        return dot3(jnp.where(same[:, :96], lhs, 0.0), high, low)

    landed(amp_in.at[pl.ds(0, 7)], 5)
    mine = total(amp_in)
    centre, rim = mine[0:4], mine[4:8]
    above = jnp.where(place < 3, pltpu.roll(centre, 127, 1), pltpu.roll(rim, 3, 1))
    below = jnp.where(place > 0, pltpu.roll(centre, 1, 1), pltpu.roll(rim, 125, 1))
    inner = applied([centre, above, below], (slice(0, 32), slice(128, 192)))
    for r in range(16):
        result[r] = local[2 * MODES + r] - inner[4 * r : 4 * r + 4]
    landed(side_in, 7)
    outer = applied([total(side_in.at[d]) for d in range(3)], (slice(32, 128),))
    for r in range(16):
        result[r] -= outer[4 * r : 4 * r + 4]
    everything = t_high.at[pl.ds(0, 704)]
    pltpu.make_async_copy(everything, everything, send_sem).wait()


def body(multipliers, own_modes, neighbour_modes, face_index, neighbour_list, coarse_factor):
    anywhere = pl.BlockSpec(memory_space=pltpu.HBM)
    rows, columns = coarse_factor.shape
    width = face_index.shape[1]
    return pl.pallas_call(
        kernel,
        out_shape=pltpu.VMEM(multipliers.shape, F32),
        in_specs=[anywhere] * 6,
        out_specs=pl.BlockSpec(memory_space=pltpu.VMEM),
        scratch_shapes=[
            pltpu.VMEM((2 * MODES + 16, 4, width), F32),
            pltpu.VMEM(face_index.shape, jnp.int32),
            pltpu.VMEM((NFACE, 2048), jnp.int32),
            pltpu.VMEM((rows, columns), F32),
            pltpu.VMEM((192, width), BF16),
            pltpu.VMEM((192, width), BF16),
            pltpu.VMEM((256, columns), BF16),
            pltpu.VMEM((256, columns), BF16),
            pltpu.VMEM((columns, 256), BF16),
            pltpu.VMEM((columns, 256), BF16),
            pltpu.VMEM((4, 4, 128), F32),
            pltpu.VMEM((5, 4, 128), F32),
            pltpu.VMEM((8, 4, 128), F32),
            pltpu.VMEM((8, 8, 384), F32),
            pltpu.VMEM((8, 8, 384), F32),
            pltpu.VMEM((8, 8, 384), F32),
            pltpu.VMEM((8, 8, 384), F32),
            pltpu.VMEM((8, 8, 128), F32),
            pltpu.VMEM((8, 8, 128), F32),
            pltpu.VMEM((8, 4, 128), F32),
            pltpu.VMEM((3, 8, 4, 128), F32),
            pltpu.VMEM((16, columns), F32),
            pltpu.SemaphoreType.DMA((4,)),
            pltpu.SemaphoreType.DMA,
            pltpu.SemaphoreType.DMA((8,)),
            pltpu.SemaphoreType.REGULAR((3,)),
        ],
        compiler_params=pltpu.CompilerParams(collective_id=0, has_side_effects=True),
    )(multipliers, own_modes, neighbour_modes, face_index, neighbour_list.T, coarse_factor)


def solution(mesh):
    placed = (
        P(None, ("sub", "crs"), None),
        P(None, ("sub", "crs"), None),
        P(None, ("sub", "crs"), None),
        P(("sub", "crs"), None),
        P(),
        P("sub", "crs"),
    )
    return jax.shard_map(
        body, mesh=mesh, in_specs=placed, out_specs=P(None, ("sub", "crs"), None), check_vma=False
    )
```
